32 devices in a mesh: gx: 2 (over core), gy: 4 (over y, x), gz: 4 (over z).
Axes of the slice: x: 2, y: 2, z: 4, core: 2. Of those that a mesh axis runs over, the one named last changes fastest.
Arguments:
- displacement: float32 [3, 12, 24, 1536], P(None, 'gx', 'gy', 'gz'), may hold values from -0.18 to 0.18
- size_field_modes: float32 [27, 4, 8, 512], P(None, 'gx', 'gy', 'gz'), may hold values from -6 to 6
- velocity: float32 [3, 4, 8, 512], P(None, 'gx', 'gy', 'gz'), may hold values from -1 to 1
Outputs:
- advected_field: float32 [27, 4, 8, 512], P(None, 'gx', 'gy', 'gz')
- gradient: float32 [3, 12, 24, 1536], P(None, 'gx', 'gy', 'gz')
- checks: float32 [3], replicated
The draws below stay inside these ranges and needn't reach their ends.
All inputs are finite; a program needn't handle non-finite values. Where the reference program divides by a largest or mean magnitude, that divisor is 1e-20 or more.
Results may differ from the reference program's by a relative error of at most 0.0001.
Values sent between devices are 32-bit elements; how exact they have to be, the bound alone decides.
A program may use at most 64 MiB of HBM per device.

```python
import math
import jax
import jax.numpy as jnp
import numpy as np
from jax import lax

LOCAL_ELEMS_X = 2
LOCAL_ELEMS_Y = 2
LOCAL_ELEMS_Z = 128
SUBSTEPS = 4
GLOBAL_ELEMS_X = 4
GLOBAL_ELEMS_Y = 8
GLOBAL_ELEMS_Z = 512
ELEMENTS = 16384


def draw_size_field_modes(key, part):
    random_key_noise, random_key_blocks = jax.random.split(key)
    noise_component = jnp.clip(0.5 * jax.random.normal(random_key_noise, (27, GLOBAL_ELEMS_X, GLOBAL_ELEMS_Y, GLOBAL_ELEMS_Z), jnp.float32), -3.0, 3.0)
    block_list = jax.random.uniform(random_key_blocks, (GLOBAL_ELEMS_X // LOCAL_ELEMS_X, GLOBAL_ELEMS_Y // LOCAL_ELEMS_Y, GLOBAL_ELEMS_Z // LOCAL_ELEMS_Z), jnp.float32, -3.0, 3.0)
    offset = jnp.repeat(jnp.repeat(jnp.repeat(block_list, LOCAL_ELEMS_X, axis=0), LOCAL_ELEMS_Y, axis=1), LOCAL_ELEMS_Z, axis=2)
    return noise_component.at[0].add(offset)


def draw_velocity(key, part):
    random_key_heading, random_key_scale = jax.random.split(key)
    heading_text = jax.random.uniform(random_key_heading, (3, GLOBAL_ELEMS_X, GLOBAL_ELEMS_Y, GLOBAL_ELEMS_Z), jnp.float32, -1.0, 1.0)
    scale_factors = jnp.exp(jax.random.uniform(random_key_scale, (GLOBAL_ELEMS_X // LOCAL_ELEMS_X, GLOBAL_ELEMS_Y // LOCAL_ELEMS_Y, GLOBAL_ELEMS_Z // LOCAL_ELEMS_Z), jnp.float32, math.log(0.15), 0.0))
    expanded = jnp.repeat(jnp.repeat(jnp.repeat(scale_factors, LOCAL_ELEMS_X, axis=0), LOCAL_ELEMS_Y, axis=1), LOCAL_ELEMS_Z, axis=2)
    return heading_text * expanded[None]


def block_levels(rng, shape, shards, low, largest):
    gain = 1.0
    for axis_at, blocks in shards:
        draws = jax.random.uniform(jax.random.fold_in(jax.random.fold_in(rng, 6), axis_at), (blocks,), jnp.float32, low / len(shards), largest / len(shards))
        gain = gain * jnp.repeat(jnp.exp(draws), shape[axis_at] // blocks).reshape((-1,) + (1,) * (len(shape) - 1 - axis_at))
    return gain


def normal_values(own_key, shape, scale, most, cuts=(), kind=jnp.bfloat16):
    drawn = jax.random.normal(own_key, shape, jnp.float32) * scale
    if len(cuts) > 0:
        drawn = block_levels(own_key, shape, cuts, -0.22, 0.18) * drawn
    return jnp.clip(drawn, min=-most, max=most).astype(kind)


def setup_inputs(seed: int = 0) -> dict:
    key_list = jax.random.split(jax.random.key(seed), 4)
    displacement = normal_values(key_list[0], (3, 3 * GLOBAL_ELEMS_X, 3 * GLOBAL_ELEMS_Y, 3 * GLOBAL_ELEMS_Z), 0.03, 0.18, ((1, 2), (2, 4), (3, 4)), jnp.float32)
    size_field_modes = draw_size_field_modes(jax.random.fold_in(key_list[3], 71), 0)
    velocity = draw_velocity(jax.random.fold_in(key_list[3], 71), 0)
    return {"displacement": displacement, "size_field_modes": size_field_modes, "velocity": velocity}


root_half = 0.7071067811865476
root_three_half = 1.224744871391589
root_five_half = 1.5811388300841898
plus_values = (0.7071067811865476, 1.224744871391589, 1.5811388300841898)
minus_values = (0.7071067811865476, -1.224744871391589, 1.5811388300841898)
stiffness = ((0.0, 0.0, 0.0), (1.7320508075688772, 0.0, 0.0), (0.0, 3.872983346207417, 0.0))
courant = 0.1
theta_size = 0.3
trial_step = 0.05

def build_tables():
    points = np.array([-0.8611363115940526, -0.3399810435848563, 0.3399810435848563, 0.8611363115940526])
    weights = np.array([0.3478548451374538, 0.6521451548625461, 0.6521451548625461, 0.3478548451374538])
    points = 0.5 * (points + 1.0)
    weights = 0.5 * weights
    node_points = np.array([0.0, 1.0 / 3.0, 2.0 / 3.0, 1.0])
    value_table = np.zeros((4, 4))
    slope_table = np.zeros((4, 4))
    for column in range(4):
        others = [node_points[member] for member in range(4) if member != column]
        denominator = np.prod([node_points[column] - member for member in others])
        for quad_row in range(4):
            gauss_point = points[quad_row]
            value_table[quad_row, column] = np.prod([gauss_point - member for member in others]) / denominator
            slope_table[quad_row, column] = sum((np.prod([gauss_point - others[position] for position in range(3) if position != skipped]) for skipped in range(3))) / denominator
    centred = 2.0 * points - 1.0
    legendre_table = np.stack([np.full(4, root_half), root_three_half * centred, root_five_half * 0.5 * (3.0 * centred ** 2 - 1.0)], axis=1)
    cube_table = (weights[:, None, None] * weights[None, :, None] * weights[None, None, :]).reshape(4, 4, 4, 1, 1, 1)
    return (value_table, slope_table, legendre_table, cube_table)

def as_table(operand):
    return jnp.asarray(np.asarray(operand), jnp.float32)

def contract(weights_table, operand, along):
    product = jnp.tensordot(as_table(weights_table), operand, axes=([1], [along]), precision=lax.Precision.HIGHEST)
    return jnp.moveaxis(product, 0, along)

def trace_along(modal_coefficients, vector, direction):
    return jnp.tensordot(as_table(vector), modal_coefficients, axes=([0], [direction]), precision=lax.Precision.HIGHEST)

def spread_shape(vector, direction):
    broadcast_shape = [1] * 6
    broadcast_shape[direction] = 3
    return as_table(vector).reshape(broadcast_shape)

def boundary_terms(modal_coefficients, local_speed, right_ext, left_ext, speed_ext, direction):
    extent = modal_coefficients.shape[3 + direction]
    face_speed = 0.5 * (lax.slice_in_dim(speed_ext, 0, extent + 1, axis=direction) + lax.slice_in_dim(speed_ext, 1, extent + 2, axis=direction))
    flux = jnp.maximum(face_speed, 0.0)[None, None] * right_ext + jnp.minimum(face_speed, 0.0)[None, None] * left_ext
    flux_left = lax.slice_in_dim(flux, 0, extent, axis=2 + direction)
    flux_right = lax.slice_in_dim(flux, 1, extent + 1, axis=2 + direction)
    lifted = contract(stiffness, modal_coefficients, direction)
    faces = spread_shape(plus_values, direction) * jnp.expand_dims(flux_right, direction) - spread_shape(minus_values, direction) * jnp.expand_dims(flux_left, direction)
    return local_speed[None, None, None] * lifted - faces

def element_energy(corners, modal_coefficients):
    lagrange_values, lagrange_slopes, legendre_values, cube_weights = build_tables()
    along_value = contract(lagrange_values, corners, 1)
    along_slope = contract(lagrange_slopes, corners, 1)
    value_value = contract(lagrange_values, along_value, 2)
    jac_first = contract(lagrange_values, contract(lagrange_values, along_slope, 2), 3)
    jac_second = contract(lagrange_values, contract(lagrange_slopes, along_value, 2), 3)
    jac_third = contract(lagrange_slopes, value_value, 3)
    columns = (jac_first, jac_second, jac_third)
    sample = contract(legendre_values, contract(legendre_values, contract(legendre_values, modal_coefficients, 0), 1), 2)
    target_size = jnp.exp(theta_size * sample)
    inverse = 1.0 / target_size
    mapped = [[((1.0 if component == column else 0.0) + columns[column][component]) * inverse for column in range(3)] for component in range(3)]
    metric = jnp.zeros_like(sample)
    for first_column in range(3):
        for second_column in range(3):
            gram_entry = mapped[0][first_column] * mapped[0][second_column] + mapped[1][first_column] * mapped[1][second_column] + mapped[2][first_column] * mapped[2][second_column]
            deviation = gram_entry - (1.0 if first_column == second_column else 0.0)
            metric = metric + deviation * deviation
    return jnp.sum(as_table(cube_weights) * target_size ** 3 * metric)

def element_corners(padded):
    gathered = padded
    for along, stack_axis in ((1, 1), (3, 2), (5, 3)):
        extent = (gathered.shape[along] - 1) // 3
        gathered = jnp.stack([lax.slice_in_dim(gathered, node_offset, node_offset + 3 * extent - 2, stride=3, axis=along) for node_offset in range(4)], axis=stack_axis)
    return gathered

def pad_one(operand, node_offset, along):
    config = [(0, 0, 0)] * operand.ndim
    config[along] = (node_offset, 3 - node_offset, 2)
    return lax.pad(operand, jnp.zeros((), operand.dtype), config)

def spread_corners(corner_grad):
    spread = corner_grad
    for stack_axis, along in ((3, 5), (2, 3), (1, 1)):
        pieces = [pad_one(lax.index_in_dim(spread, node_offset, axis=stack_axis, keepdims=False), node_offset, along) for node_offset in range(4)]
        spread = pieces[0] + pieces[1] + pieces[2] + pieces[3]
    return spread

def advection_rate(modal_coefficients, velocity):
    accumulated = jnp.zeros_like(modal_coefficients)
    for direction in range(3):
        element_axis = 2 + direction
        extent = modal_coefficients.shape[3 + direction]
        local_speed = velocity[direction]
        speed_ext = jnp.concatenate([lax.slice_in_dim(local_speed, extent - 1, extent, axis=direction), local_speed, lax.slice_in_dim(local_speed, 0, 1, axis=direction)], axis=direction)
        right_trace = trace_along(modal_coefficients, plus_values, direction)
        left_trace = trace_along(modal_coefficients, minus_values, direction)
        right_ext = jnp.concatenate([lax.slice_in_dim(right_trace, extent - 1, extent, axis=element_axis), right_trace], axis=element_axis)
        left_ext = jnp.concatenate([left_trace, lax.slice_in_dim(left_trace, 0, 1, axis=element_axis)], axis=element_axis)
        accumulated = accumulated + boundary_terms(modal_coefficients, local_speed, right_ext, left_ext, speed_ext, direction)
    return 2.0 * accumulated

def periodic_pad(nodal):
    for along in (1, 2, 3):
        nodal = jnp.concatenate([nodal, lax.slice_in_dim(nodal, 0, 1, axis=along)], axis=along)
    return nodal

def periodic_fold(gradient_pad):
    for along in (1, 2, 3):
        extent = gradient_pad.shape[along] - 1
        gradient_pad = jnp.concatenate([lax.slice_in_dim(gradient_pad, 0, 1, axis=along) + lax.slice_in_dim(gradient_pad, extent, extent + 1, axis=along), lax.slice_in_dim(gradient_pad, 1, extent, axis=along)], axis=along)
    return gradient_pad

def gradient_scan(padded, modal_coefficients):

    def advance(running, slab_start):
        energy_sum, gradient_pad = running
        nodes_slab = lax.dynamic_slice_in_dim(padded, 3 * slab_start, 4, axis=1)
        field_slab = lax.dynamic_slice_in_dim(modal_coefficients, slab_start, 1, axis=3)
        energy_here, corner_grad = jax.value_and_grad(element_energy)(element_corners(nodes_slab), field_slab)
        contribution = spread_corners(corner_grad)
        current = lax.dynamic_slice_in_dim(gradient_pad, 3 * slab_start, 4, axis=1)
        gradient_pad = lax.dynamic_update_slice_in_dim(gradient_pad, current + contribution, 3 * slab_start, axis=1)
        return ((energy_sum + energy_here, gradient_pad), None)
    start_value = (jnp.zeros((), jnp.float32), jnp.zeros_like(padded))
    finished, unused = lax.scan(advance, start_value, jnp.arange(GLOBAL_ELEMS_X, dtype=jnp.int32))
    return finished

def energy_scan(padded, modal_coefficients):

    def advance(energy_sum, slab_start):
        nodes_slab = lax.dynamic_slice_in_dim(padded, 3 * slab_start, 4, axis=1)
        field_slab = lax.dynamic_slice_in_dim(modal_coefficients, slab_start, 1, axis=3)
        return (energy_sum + element_energy(element_corners(nodes_slab), field_slab), None)
    finished, unused = lax.scan(advance, jnp.zeros((), jnp.float32), jnp.arange(GLOBAL_ELEMS_X, dtype=jnp.int32))
    return finished

def reference(displacement, size_field_modes, velocity):
    modal_coefficients = size_field_modes.reshape(3, 3, 3, GLOBAL_ELEMS_X, GLOBAL_ELEMS_Y, GLOBAL_ELEMS_Z)
    fastest = jnp.max(lax.optimization_barrier(jnp.sum(jnp.abs(velocity), axis=0)))
    time_step = courant / jnp.maximum(fastest, 0.25)
    for substep in range(SUBSTEPS):
        midway = modal_coefficients + time_step * advection_rate(modal_coefficients, velocity)
        modal_coefficients = 0.5 * modal_coefficients + 0.5 * (midway + time_step * advection_rate(midway, velocity))
    energy_total, gradient_pad = gradient_scan(periodic_pad(displacement), modal_coefficients)
    gradient = periodic_fold(gradient_pad)
    elements = 1.0 * ELEMENTS
    entries = 81.0 * ELEMENTS
    square_total = jnp.sum(gradient * gradient)
    step_length = trial_step / jnp.sqrt(1.0 + square_total / entries)
    trial_nodes = displacement - step_length * gradient
    trial_total = energy_scan(periodic_pad(trial_nodes), modal_coefficients)
    checks = jnp.stack([energy_total / elements, square_total / entries, trial_total / elements])
    return (modal_coefficients.reshape(27, GLOBAL_ELEMS_X, GLOBAL_ELEMS_Y, GLOBAL_ELEMS_Z), gradient, checks)
```

```python
import functools

import jax
import jax.numpy as jnp
import numpy as np
from jax import lax
from jax.experimental import pallas as pl
from jax.experimental.pallas import tpu as pltpu
from jax.sharding import PartitionSpec as P

SUBSTEPS = 4
MESH = pl.DeviceIdType.MESH
AXES = ("gx", "gy", "gz")

plus_values = (0.7071067811865476, 1.224744871391589, 1.5811388300841898)
g10 = 1.7320508075688772
g21 = 3.872983346207417
courant = 0.1
theta_size = 0.3
trial_step = 0.05


def tables_1d():
    points = np.array(
        [-0.8611363115940526, -0.3399810435848563, 0.3399810435848563, 0.8611363115940526]
    )
    weights = np.array(
        [0.3478548451374538, 0.6521451548625461, 0.6521451548625461, 0.3478548451374538]
    )
    points = 0.5 * (points + 1.0)
    weights = 0.5 * weights
    nodes = np.array([0.0, 1.0 / 3.0, 2.0 / 3.0, 1.0])
    value = np.zeros((4, 4))
    slope = np.zeros((4, 4))
    for m in range(4):
        others = [nodes[o] for o in range(4) if o != m]
        den = np.prod([nodes[m] - o for o in others])
        for q in range(4):
            g = points[q]
            value[q, m] = np.prod([g - o for o in others]) / den
            slope[q, m] = (
                sum(np.prod([g - others[t] for t in range(3) if t != s]) for s in range(3)) / den
            )
    c = 2.0 * points - 1.0
    legendre = np.stack(
        [
            np.full(4, plus_values[0]),
            plus_values[1] * c,
            plus_values[2] * 0.5 * (3.0 * c**2 - 1.0),
        ],
        axis=1,
    )
    return value, slope, legendre, weights


def row_tables(Y, Z):
    value, slope, legendre, weights = tables_1d()
    rows, nodes = 4 * Y, 3 * Y + 1
    tv = np.zeros((rows, rows))
    td = np.zeros((rows, rows))
    for e in range(Y):
        tv[4 * e : 4 * e + 4, 3 * e : 3 * e + 4] = value
        td[4 * e : 4 * e + 4, 3 * e : 3 * e + 4] = slope
    blocks = [tv[:, j] for j in range(nodes)] + [td[:, j] for j in range(nodes)]
    blocks += [tv[s, :] for s in range(rows)] + [td[s, :] for s in range(rows)]
    for b in range(3):
        for e in range(Y):
            col = np.zeros(rows)
            col[4 * e : 4 * e + 4] = legendre[:, b]
            blocks.append(col)
    blocks.append(np.tile(weights, Y))
    stacked = np.stack(blocks).astype(np.float32)
    return np.ascontiguousarray(np.broadcast_to(stacked[:, :, None], stacked.shape + (Z,)))


def kernel(sizes, X, Y, Z, disp, modes, vel, tab, adv, grad, checks,
           perm, slab, U, W, VEL, FS, SX, RX, SY, RY, SZ, RZ,
           RED, REDR, N, GN, A, G, B, SIZ,
           NXR, NYS, NYR, NZS, NZR, FXR, FYS, FYR, FZS, FZR,
           hs, hr, rs, rr, ns, nr, fs, fr):
    value, slope, legendre, weights = tables_1d()
    NX, NY = 3 * X, 3 * Y
    ROWS = 4 * Y
    EL = X * Y
    f32 = jnp.float32
    index = [lax.axis_index(a) for a in AXES]
    lane = lax.broadcasted_iota(jnp.int32, (ROWS, Z), 1)
    row = lax.broadcasted_iota(jnp.int32, (ROWS, Z), 0)
    oTV, oTD, oGV, oGD, oL, oW = 0, NY + 1, 2 * NY + 2, 2 * NY + 2 + ROWS, 2 * NY + 2 + 2 * ROWS, 2 * NY + 2 + 2 * ROWS + 3 * Y

    def at(axis, by):
        n = sizes[axis]
        return {AXES[axis]: lax.rem(index[axis] + (by + n), n)}

    barrier = pltpu.get_barrier_semaphore()
    total = 0
    for axis in range(3):
        for by in range(1, sizes[axis]):
            pl.semaphore_signal(barrier, inc=1, device_id=at(axis, by), device_id_type=MESH)
            total += 1

    def copy(src, dst, ss, sr, axis, by):
        return pltpu.make_async_remote_copy(
            src_ref=src, dst_ref=dst, send_sem=ss, recv_sem=sr,
            device_id=at(axis, by), device_id_type=MESH,
        )

    U[...] = jnp.zeros_like(U)
    VEL[...] = jnp.zeros_like(VEL)
    for ix in range(X):
        U[:, ix * Y : ix * Y + Y, :] = modes[:, ix]
        VEL[:, ix * Y : ix * Y + Y, :] = vel[:, ix]
    RED[0, 0] = jnp.zeros((2, ROWS, Z), f32)
    RED[0, 0, 0] = jnp.abs(VEL[0]) + jnp.abs(VEL[1]) + jnp.abs(VEL[2])
    a_i = lax.broadcasted_iota(jnp.int32, (3 * Z, 3 * Z), 0)
    b_i = lax.broadcasted_iota(jnp.int32, (3 * Z, 3 * Z), 1)
    b_k = (b_i >= Z).astype(jnp.int32) + (b_i >= 2 * Z).astype(jnp.int32)
    perm[...] = (a_i == 3 * (b_i - b_k * Z) + b_k).astype(f32)
    slab[...] = jnp.zeros_like(slab)
    for c in range(3):
        for i in range(NX):
            slab[c * NX + i, 0:NY, :] = disp[c, i]
    spread = jnp.dot(
        slab[...].reshape(3 * NX * ROWS, 3 * Z), perm[...],
        precision=lax.Precision.HIGHEST, preferred_element_type=f32,
    ).reshape(3, NX, ROWS, 3 * Z)
    for c in range(3):
        for k in range(3):
            N[c, 0:NX, k] = spread[c, :, :, k * Z : (k + 1) * Z]

    pl.semaphore_wait(barrier, total)

    def red_copies(r, axis):
        off = sum(sizes[t] - 1 for t in range(axis))
        return [
            copy(RED.at[r, axis], REDR.at[r, off + by - 1], rs.at[r, off + by - 1], rr.at[r, off + by - 1], axis, by)
            for by in range(1, sizes[axis])
        ]

    def red_start(r, axis):
        for cp in red_copies(r, axis):
            cp.start()

    def red_finish(r, axis, op):
        off = sum(sizes[t] - 1 for t in range(axis))
        for cp in red_copies(r, axis):
            cp.wait()
        total = RED[r, axis]
        for by in range(1, sizes[axis]):
            total = op(total, REDR[r, off + by - 1])
        RED[r, axis + 1] = total

    def rim_x(a, t):
        return copy(a.at[:, 0, 0:3], NXR.at[t], ns.at[t, 0], nr.at[t, 0], 0, -1)

    def rim_y(t):
        return copy(NYS.at[t], NYR.at[t], ns.at[t, 1], nr.at[t, 1], 1, -1)

    def rim_y_pack(a, t):
        for c in range(3):
            for k in range(3):
                a[c, NX, k] = NXR[t, c, k]
        for c in range(3):
            for i in range(NX + 1):
                for k in range(3):
                    NYS[t, c, i, k : k + 1, :] = a[c, i, k, 0:1, :]

    def rim_y_unpack(a, t):
        for c in range(3):
            for i in range(NX + 1):
                for k in range(3):
                    a[c, i, k, NY : NY + 1, :] = NYR[t, c, i, k : k + 1, :]

    def rim_z(t):
        return copy(NZS.at[t], NZR.at[t], ns.at[t, 2], nr.at[t, 2], 2, -1)

    def rim_z_pack(a, t):
        packed = jnp.zeros((ROWS, Z), f32)
        for c in range(3):
            for i in range(NX + 1):
                packed = jnp.where(lane == c * (NX + 1) + i, a[c, i, 0][:, 0:1], packed)
        NZS[t] = packed

    def rim_z_unpack(a, t):
        packed = NZR[t]
        for c in range(3):
            for i in range(NX + 1):
                at_ = c * (NX + 1) + i
                a[c, i, 3] = jnp.where(lane == Z - 1, packed[:, at_ : at_ + 1], pltpu.roll(a[c, i, 0], Z - 1, 1))

    def halo_copies(s):
        out = []
        for d, (sb, rb) in enumerate(((SX, RX), (SY, RY), (SZ, RZ))):
            for way in range(2):
                out.append(copy(sb.at[s, way], rb.at[s, way], hs.at[s, 2 * d + way], hr.at[s, 2 * d + way], d, 1 - 2 * way))
        return out

    def send_parts(s, n, tp, tm):
        SX[s, 0, n] = tp[0][(X - 1) * Y : EL]
        SX[s, 1, n] = tm[0][0:Y]
        for ix in range(X):
            SY[s, 0, n, ix : ix + 1] = tp[1][ix * Y + Y - 1 : ix * Y + Y]
            SY[s, 1, n, ix : ix + 1] = tm[1][ix * Y : ix * Y + 1]

    def prev_of(d, t, s, n):
        if d == 0:
            return jnp.concatenate([RX[s, 0, n], t[: ROWS - Y]], axis=0)
        if d == 1:
            parts = []
            for ix in range(X):
                parts += [RY[s, 0, n, ix : ix + 1], t[ix * Y : ix * Y + Y - 1]]
            return jnp.concatenate(parts + [t[EL:]], axis=0)
        return jnp.where(lane == 0, RZ[s, 0][:, n : n + 1], pltpu.roll(t, 1, 1))

    def next_of(d, t, s, n):
        if d == 0:
            return jnp.concatenate([t[Y:EL], RX[s, 1, n], t[EL:]], axis=0)
        if d == 1:
            parts = []
            for ix in range(X):
                parts += [t[ix * Y + 1 : ix * Y + Y], RY[s, 1, n, ix : ix + 1]]
            return jnp.concatenate(parts + [t[EL:]], axis=0)
        return jnp.where(lane == Z - 1, RZ[s, 1][:, n : n + 1], pltpu.roll(t, Z - 1, 1))

    strides = (9, 3, 1)
    others = [[m for m in range(27) if (m // strides[d]) % 3 == 0] for d in range(3)]

    def rate(src, s, first, between):
        u = [src[m] for m in range(27)]
        tp, tm = [[], [], []], [[], [], []]
        for d in range(3):
            for m in others[d]:
                even = plus_values[0] * u[m] + plus_values[2] * u[m + 2 * strides[d]]
                odd = plus_values[1] * u[m + strides[d]]
                tp[d].append(even + odd)
                tm[d].append(even - odd)
        up, low = jnp.zeros((ROWS, Z), f32), jnp.zeros((ROWS, Z), f32)
        for n in range(9):
            send_parts(s, n, [tp[d][n] for d in range(3)], [tm[d][n] for d in range(3)])
            up = jnp.where(lane == n, tp[2][n][:, Z - 1 : Z], up)
            low = jnp.where(lane == n, tm[2][n][:, 0:1], low)
        v = [VEL[d] for d in range(3)]
        send_parts(s, 9, v, v)
        if first:
            up = jnp.where(lane == 9, v[2][:, Z - 1 : Z], up)
            low = jnp.where(lane == 9, v[2][:, 0:1], low)
        SZ[s, 0] = up
        SZ[s, 1] = low
        for cp in halo_copies(s):
            cp.start()
        acc = [None] * 27
        for d in range(3):
            st = strides[d]
            va, vb = (2.0 * g10) * v[d], (2.0 * g21) * v[d]
            for m in others[d]:
                for mm, term in ((m + st, va * u[m]), (m + 2 * st, vb * u[m + st])):
                    acc[mm] = term if acc[mm] is None else acc[mm] + term
        between()
        for cp in halo_copies(s):
            cp.wait()
        if first:
            for d in range(3):
                high = v[d] + next_of(d, v[d], s, 9)
                lowf = prev_of(d, v[d], s, 9) + v[d]
                FS[d, 0] = jnp.maximum(high, 0.0)
                FS[d, 1] = jnp.minimum(high, 0.0)
                FS[d, 2] = jnp.maximum(lowf, 0.0)
                FS[d, 3] = jnp.minimum(lowf, 0.0)
        for d in range(3):
            st = strides[d]
            hp, hm, lp, lm = [FS[d, t] for t in range(4)]
            for n, m in enumerate(others[d]):
                hi = hp * tp[d][n] + hm * next_of(d, tm[d][n], s, n)
                lo = lp * prev_of(d, tp[d][n], s, n) + lm * tm[d][n]
                diff, both = lo - hi, lo + hi
                for mm, term in (
                    (m, plus_values[0] * diff),
                    (m + st, (-plus_values[1]) * both),
                    (m + 2 * st, plus_values[2] * diff),
                ):
                    acc[mm] = term if acc[mm] is None else acc[mm] + term
        return acc

    red_start(0, 0)
    rim_x(N, 0).start()

    def first_between():
        red_finish(0, 0, jnp.maximum)
        red_start(0, 1)
        rim_x(N, 0).wait()
        rim_y_pack(N, 0)
        rim_y(0).start()

    def second_between():
        red_finish(0, 1, jnp.maximum)
        red_start(0, 2)
        rim_y(0).wait()
        rim_y_unpack(N, 0)
        rim_z_pack(N, 0)
        rim_z(0).start()

    w1 = rate(U, 0, True, first_between)
    for m in range(27):
        W[m] = w1[m]
    w2 = rate(W, 1, False, second_between)
    red_finish(0, 2, jnp.maximum)
    rim_z(0).wait()
    rim_z_unpack(N, 0)
    fastest = jnp.max(RED[0, 3, 0], axis=(0, 1), keepdims=True)
    dt = courant / jnp.maximum(fastest, 0.25)
    dt = jnp.broadcast_to(dt, (ROWS, Z))
    half = 0.5 * dt * dt
    for m in range(27):
        U[m] = U[m] + dt * W[m] + half * w2[m]

    def substep(t, carry):
        w = rate(U, 2 * t, False, lambda: None)
        for m in range(27):
            W[m] = w[m]
        w = rate(W, 2 * t + 1, False, lambda: None)
        for m in range(27):
            U[m] = U[m] + dt * W[m] + half * w[m]
        return carry

    lax.fori_loop(1, SUBSTEPS, substep, 0)
    for ix in range(X):
        adv[:, ix] = U[:, ix * Y : ix * Y + Y, :]

    def size_of(ix, carry):
        mid = {}
        for a in range(3):
            for r in range(4):
                mid[a, r] = None
            for c in range(3):
                t = None
                for b in range(3):
                    for e in range(Y):
                        term = tab[oL + b * Y + e] * U[a * 9 + b * 3 + c, pl.ds(ix * Y + e, 1), :]
                        t = term if t is None else t + term
                for r in range(4):
                    term = float(legendre[r, c]) * t
                    mid[a, r] = term if mid[a, r] is None else mid[a, r] + term
        for p in range(4):
            for r in range(4):
                s = sum(float(legendre[p, a]) * mid[a, r] for a in range(3))
                SIZ[ix, p, r] = jnp.exp(theta_size * s)
        return carry

    lax.fori_loop(0, X, size_of, 0)

    def energy(with_grad):
        def yz(i, carry):
            for c in range(3):
                yv, yd = [], []
                for k in range(4):
                    sv = sd = None
                    for j in range(NY + 1):
                        x = N[c, i, k, j : j + 1, :]
                        tv, td = tab[oTV + j] * x, tab[oTD + j] * x
                        sv = tv if sv is None else sv + tv
                        sd = td if sd is None else sd + td
                    yv.append(sv)
                    yd.append(sd)
                for r in range(4):
                    A[0, c, i, r] = sum(float(value[r, k]) * yv[k] for k in range(4))
                    A[1, c, i, r] = sum(float(value[r, k]) * yd[k] for k in range(4))
                    A[2, c, i, r] = sum(float(slope[r, k]) * yv[k] for k in range(4))
            return carry

        lax.fori_loop(0, NX + 1, yz, 0)
        wrow = tab[oW]

        def gauss(t, esum):
            ix, r = t // 4, t % 4
            wr = jnp.where((r == 0) | (r == 3), float(weights[0]), float(weights[1]))
            for p in range(4):
                size = SIZ[ix, p, r]
                inv = 1.0 / size
                M = [[None] * 3 for _ in range(3)]
                for c in range(3):
                    for d in range(3):
                        tb = slope if d == 0 else value
                        jac = sum(float(tb[p, m]) * A[d, c, 3 * ix + m, r] for m in range(4))
                        if c == d:
                            jac = jac + 1.0
                        M[c][d] = jac * inv
                D = [[None] * 3 for _ in range(3)]
                metric = None
                for d in range(3):
                    for e in range(d, 3):
                        dev = M[0][d] * M[0][e] + M[1][d] * M[1][e] + M[2][d] * M[2][e]
                        if d == e:
                            dev = dev - 1.0
                        D[d][e] = D[e][d] = dev
                        sq = dev * dev
                        if d != e:
                            sq = 2.0 * sq
                        metric = sq if metric is None else metric + sq
                w = wrow * (wr * float(weights[p]))
                size2 = size * size
                esum = esum + w * (size2 * size) * metric
                if with_grad:
                    scale = (4.0 * w) * size2
                    for c in range(3):
                        for d in range(3):
                            g = M[c][0] * D[0][d] + M[c][1] * D[1][d] + M[c][2] * D[2][d]
                            G[d, c, ix, p, r] = scale * g
            return esum

        return lax.fori_loop(0, 4 * X, gauss, jnp.zeros((ROWS, Z), f32))

    esum = energy(True)

    def back_c(c, carry):
        for i in range(NX + 1):
            bv = [None] * 4
            bd = [None] * 4
            for r in range(4):
                ga = []
                for d in range(3):
                    tb = slope if d == 0 else value
                    acc = None
                    for ix in range(X):
                        m = i - 3 * ix
                        if 0 <= m <= 3:
                            for p in range(4):
                                term = float(tb[p, m]) * G[d, c, ix, p, r]
                                acc = term if acc is None else acc + term
                    ga.append(acc)
                for k in range(4):
                    tv = float(value[r, k]) * ga[0] + float(slope[r, k]) * ga[2]
                    td = float(value[r, k]) * ga[1]
                    bv[k] = tv if bv[k] is None else bv[k] + tv
                    bd[k] = td if bd[k] is None else bd[k] + td
            for k in range(4):
                B[0, i, k] = bv[k]
                B[1, i, k] = bd[k]
        for i in range(NX + 1):
            for k in range(4):
                acc = None
                for s in range(ROWS):
                    term = tab[oGV + s] * B[0, i, k, s : s + 1, :] + tab[oGD + s] * B[1, i, k, s : s + 1, :]
                    acc = term if acc is None else acc + term
                GN[c, i, k] = acc
        return carry

    lax.fori_loop(0, 3, back_c, 0)

    packed = jnp.zeros((ROWS, Z), f32)
    for c in range(3):
        for i in range(NX + 1):
            packed = jnp.where(lane == c * (NX + 1) + i, GN[c, i, 3][:, Z - 1 : Z], packed)
    FZS[...] = packed
    cz = copy(FZS, FZR, fs.at[0], fr.at[0], 2, 1)
    cz.start()
    cz.wait()
    packed = FZR[...]
    for c in range(3):
        for i in range(NX + 1):
            at_ = c * (NX + 1) + i
            GN[c, i, 0] = GN[c, i, 0] + jnp.where(lane == 0, packed[:, at_ : at_ + 1], pltpu.roll(GN[c, i, 3], 1, 1))
    cx = copy(GN.at[:, NX, 0:3], FXR, fs.at[1], fr.at[1], 0, 1)
    cx.start()
    cx.wait()
    for c in range(3):
        for k in range(3):
            GN[c, 0, k] = GN[c, 0, k] + FXR[c, k]
    for c in range(3):
        for i in range(NX):
            for k in range(3):
                FYS[c, i, k : k + 1, :] = GN[c, i, k, NY : NY + 1, :]
    cy = copy(FYS, FYR, fs.at[2], fr.at[2], 1, 1)
    cy.start()
    cy.wait()
    ssum = jnp.zeros((ROWS, Z), f32)
    for c in range(3):
        for i in range(NX):
            for k in range(3):
                GN[c, i, k, 0:1, :] = GN[c, i, k, 0:1, :] + FYR[c, i, k : k + 1, :]
    for c in range(3):
        for i in range(NX):
            for k in range(3):
                g = GN[c, i, k]
                ssum = ssum + g * g
    ssum = jnp.where(row < NY, ssum, 0.0)
    RED[1, 0, 0] = esum
    RED[1, 0, 1] = ssum
    red_start(1, 0)
    rim_x(GN, 1).start()
    red_finish(1, 0, jnp.add)
    red_start(1, 1)
    rim_x(GN, 1).wait()
    rim_y_pack(GN, 1)
    rim_y(1).start()
    for c in range(3):
        for k in range(3):
            slab[c * NX : (c + 1) * NX, :, k * Z : (k + 1) * Z] = GN[c, 0:NX, k]
    woven = lax.dot_general(
        slab[...].reshape(3 * NX * ROWS, 3 * Z), perm[...], (((1,), (1,)), ((), ())),
        precision=lax.Precision.HIGHEST, preferred_element_type=f32,
    ).reshape(3, NX, ROWS, 3 * Z)
    grad[...] = woven[:, :, 0:NY, :]
    red_finish(1, 1, jnp.add)
    red_start(1, 2)
    rim_y(1).wait()
    rim_y_unpack(GN, 1)
    rim_z_pack(GN, 1)
    rim_z(1).start()
    red_finish(1, 2, jnp.add)
    devices = sizes[0] * sizes[1] * sizes[2]
    elements = float(EL * Z * devices)
    entries = 81.0 * elements
    etot = jnp.sum(RED[1, 3, 0], axis=(0, 1), keepdims=True)
    stot = jnp.sum(RED[1, 3, 1], axis=(0, 1), keepdims=True)
    step = jnp.broadcast_to(trial_step / jnp.sqrt(1.0 + stot / entries), (ROWS, Z))
    rim_z(1).wait()
    rim_z_unpack(GN, 1)
    for c in range(3):
        for i in range(NX + 1):
            for k in range(4):
                N[c, i, k] = N[c, i, k] - step * GN[c, i, k]
    tsum = energy(False)
    RED[2, 0, 0] = tsum
    RED[2, 0, 1] = jnp.zeros((ROWS, Z), f32)
    for axis in range(3):
        red_start(2, axis)
        red_finish(2, axis, jnp.add)
    ttot = jnp.sum(RED[2, 3, 0], axis=(0, 1), keepdims=True)
    l1 = lax.broadcasted_iota(jnp.int32, (1, Z), 1)
    checks[...] = jnp.where(
        l1 == 0, etot / elements, jnp.where(l1 == 1, stot / entries, ttot / elements)
    )


def solution(mesh):
    sizes = tuple(mesh.shape[a] for a in AXES)

    def on_device(displacement, size_field_modes, velocity):
        modes, X, Y, Z = size_field_modes.shape
        assert Y == 2 and displacement.shape == (3, 3 * X, 3 * Y, 3 * Z)
        R, NX, NY = 4 * Y, 3 * X, 3 * Y
        tab = jnp.asarray(row_tables(Y, Z))
        peers = sum(sizes) - 3
        S = 2 * SUBSTEPS
        vm = lambda *shape: pltpu.VMEM(shape, jnp.float32)
        dma = lambda *shape: pltpu.SemaphoreType.DMA(shape)
        spec = pl.BlockSpec(memory_space=pltpu.VMEM)
        adv, grad, checks = pl.pallas_call(
            functools.partial(kernel, sizes, X, Y, Z),
            out_shape=(
                jax.ShapeDtypeStruct(size_field_modes.shape, jnp.float32),
                jax.ShapeDtypeStruct(displacement.shape, jnp.float32),
                jax.ShapeDtypeStruct((1, Z), jnp.float32),
            ),
            in_specs=[spec] * 4,
            out_specs=(spec,) * 3,
            scratch_shapes=[
                vm(3 * Z, 3 * Z), vm(3 * NX, R, 3 * Z), vm(27, R, Z), vm(27, R, Z), vm(3, R, Z), vm(3, 4, R, Z),
                vm(S, 2, 10, Y, Z), vm(S, 2, 10, Y, Z), vm(S, 2, 10, X, Z), vm(S, 2, 10, X, Z),
                vm(S, 2, R, Z), vm(S, 2, R, Z),
                vm(3, 4, 2, R, Z), vm(3, peers, 2, R, Z),
                vm(3, NX + 1, 4, R, Z), vm(3, NX + 1, 4, R, Z),
                vm(3, 3, NX + 1, 4, R, Z), vm(3, 3, X, 4, 4, R, Z), vm(2, NX + 1, 4, R, Z), vm(X, 4, 4, R, Z),
                vm(2, 3, 3, R, Z), vm(2, 3, NX + 1, 3, Z), vm(2, 3, NX + 1, 3, Z), vm(2, R, Z), vm(2, R, Z),
                vm(3, 3, R, Z), vm(3, NX, 3, Z), vm(3, NX, 3, Z), vm(R, Z), vm(R, Z),
                dma(S, 6), dma(S, 6), dma(3, peers), dma(3, peers), dma(2, 3), dma(2, 3), dma(3), dma(3),
            ],
            compiler_params=pltpu.CompilerParams(collective_id=0, has_side_effects=True),
        )(displacement, size_field_modes, velocity, tab)
        return adv, grad, checks[0, 0:3]

    return jax.shard_map(
        on_device,
        mesh=mesh,
        in_specs=(P(None, "gx", "gy", "gz"),) * 3,
        out_specs=(P(None, "gx", "gy", "gz"), P(None, "gx", "gy", "gz"), P()),
        check_vma=False,
    )
```

```python
import functools

import jax
import jax.numpy as jnp
import numpy as np
from jax import lax
from jax.experimental import pallas as pl
from jax.experimental.pallas import tpu as pltpu
from jax.sharding import PartitionSpec as P

SUBSTEPS = 4
MESH = pl.DeviceIdType.MESH
AXES = ("gx", "gy", "gz")

plus_values = (0.7071067811865476, 1.224744871391589, 1.5811388300841898)
g10 = 1.7320508075688772
g21 = 3.872983346207417
courant = 0.1
theta_size = 0.3
trial_step = 0.05


def tables_1d():
    points = np.array(
        [-0.8611363115940526, -0.3399810435848563, 0.3399810435848563, 0.8611363115940526]
    )
    weights = np.array(
        [0.3478548451374538, 0.6521451548625461, 0.6521451548625461, 0.3478548451374538]
    )
    points = 0.5 * (points + 1.0)
    weights = 0.5 * weights
    nodes = np.array([0.0, 1.0 / 3.0, 2.0 / 3.0, 1.0])
    value = np.zeros((4, 4))
    slope = np.zeros((4, 4))
    for m in range(4):
        others = [nodes[o] for o in range(4) if o != m]
        den = np.prod([nodes[m] - o for o in others])
        for q in range(4):
            g = points[q]
            value[q, m] = np.prod([g - o for o in others]) / den
            slope[q, m] = (
                sum(np.prod([g - others[t] for t in range(3) if t != s]) for s in range(3)) / den
            )
    c = 2.0 * points - 1.0
    legendre = np.stack(
        [
            np.full(4, plus_values[0]),
            plus_values[1] * c,
            plus_values[2] * 0.5 * (3.0 * c**2 - 1.0),
        ],
        axis=1,
    )
    return value, slope, legendre, weights


def row_tables(Y, Z):
    value, slope, legendre, weights = tables_1d()
    rows, nodes = 4 * Y, 3 * Y + 1
    tv = np.zeros((rows, rows))
    td = np.zeros((rows, rows))
    for e in range(Y):
        tv[4 * e : 4 * e + 4, 3 * e : 3 * e + 4] = value
        td[4 * e : 4 * e + 4, 3 * e : 3 * e + 4] = slope
    blocks = [tv[:, j] for j in range(nodes)] + [td[:, j] for j in range(nodes)]
    blocks += [tv[s, :] for s in range(rows)] + [td[s, :] for s in range(rows)]
    for b in range(3):
        for e in range(Y):
            col = np.zeros(rows)
            col[4 * e : 4 * e + 4] = legendre[:, b]
            blocks.append(col)
    blocks.append(np.tile(weights, Y))
    stacked = np.stack(blocks).astype(np.float32)
    return np.ascontiguousarray(np.broadcast_to(stacked[:, :, None], stacked.shape + (Z,)))


def kernel(sizes, X, Y, Z, disp, modes, vel, tab, adv, grad, checks,
           perm, slab, U, W, VEL, FS, SX, RX, SY, RY, SZ, RZ,
           RED, REDR, N, GN, A, G, J, B, SIZ, DT,
           NXR, NYS, NYR, NZS, NZR, FXR, FYS, FYR, FZS, FZR,
           hs, hr, rs, rr, ns, nr, fs, fr):
    value, slope, legendre, weights = tables_1d()
    NX, NY = 3 * X, 3 * Y
    ROWS = 4 * Y
    EL = X * Y
    f32 = jnp.float32
    index = [lax.axis_index(a) for a in AXES]
    lane = lax.broadcasted_iota(jnp.int32, (ROWS, Z), 1)
    row = lax.broadcasted_iota(jnp.int32, (ROWS, Z), 0)
    oTV, oTD, oGV, oGD, oL, oW = 0, NY + 1, 2 * NY + 2, 2 * NY + 2 + ROWS, 2 * NY + 2 + 2 * ROWS, 2 * NY + 2 + 2 * ROWS + 3 * Y

    def at(axis, by):
        n = sizes[axis]
        return {AXES[axis]: lax.rem(index[axis] + (by + n), n)}

    barrier = pltpu.get_barrier_semaphore()
    total = 0
    moves = [(by, 0, 0) for by in range(1, sizes[0])]
    moves += [(0, b, c) for b in range(sizes[1]) for c in range(sizes[2]) if b or c]
    for move in moves:
        target = {}
        for axis in range(3):
            if move[axis]:
                target.update(at(axis, move[axis]))
        pl.semaphore_signal(barrier, inc=1, device_id=target, device_id_type=MESH)
        total += 1

    def copy(src, dst, ss, sr, axis, by):
        return pltpu.make_async_remote_copy(
            src_ref=src, dst_ref=dst, send_sem=ss, recv_sem=sr,
            device_id=at(axis, by), device_id_type=MESH,
        )

    U[...] = jnp.zeros_like(U)
    VEL[...] = jnp.zeros_like(VEL)
    for ix in range(X):
        U[:, ix * Y : ix * Y + Y, :] = modes[:, ix]
        VEL[:, ix * Y : ix * Y + Y, :] = vel[:, ix]
    RED[0, 0] = jnp.zeros_like(RED[0, 0])
    RED[0, 0, 0] = jnp.abs(VEL[0]) + jnp.abs(VEL[1]) + jnp.abs(VEL[2])
    def unweave():
        a_i = lax.broadcasted_iota(jnp.int32, (3 * Z, 3 * Z), 0)
        b_i = lax.broadcasted_iota(jnp.int32, (3 * Z, 3 * Z), 1)
        b_k = (b_i >= Z).astype(jnp.int32) + (b_i >= 2 * Z).astype(jnp.int32)
        perm[...] = (a_i == 3 * (b_i - b_k * Z) + b_k).astype(f32)
        slab[...] = jnp.zeros_like(slab)
        for c in range(3):
            for i in range(NX):
                slab[c * NX + i, 0:NY, :] = disp[c, i]
        spread = jnp.dot(
            slab[...].reshape(3 * NX * ROWS, 3 * Z), perm[...],
            precision=lax.Precision.HIGHEST, preferred_element_type=f32,
        ).reshape(3, NX, ROWS, 3 * Z)
        for c in range(3):
            for k in range(3):
                N[c, 0:NX, k] = spread[c, :, :, k * Z : (k + 1) * Z]

    pl.semaphore_wait(barrier, total)

    def peers_of(phase):
        if phase == 0:
            return [(by, 0, 0) for by in range(1, sizes[0])]
        return [(0, b, c) for b in range(sizes[1]) for c in range(sizes[2]) if b or c]

    def red_copies(r, phase):
        off = 0 if phase == 0 else sizes[0] - 1
        out = []
        for n, move in enumerate(peers_of(phase)):
            target = {}
            for axis in range(3):
                if move[axis]:
                    target.update(at(axis, move[axis]))
            out.append(pltpu.make_async_remote_copy(
                src_ref=RED.at[r, phase], dst_ref=REDR.at[r, off + n],
                send_sem=rs.at[r, off + n], recv_sem=rr.at[r, off + n],
                device_id=target, device_id_type=MESH,
            ))
        return out

    def red_start(r, phase):
        for cp in red_copies(r, phase):
            cp.start()

    def red_finish(r, phase, op):
        off = 0 if phase == 0 else sizes[0] - 1
        copies = red_copies(r, phase)
        for cp in copies:
            cp.wait()
        total = RED[r, phase]
        for n in range(len(copies)):
            total = op(total, REDR[r, off + n])
        RED[r, phase + 1] = total

    def rim_x(a, t):
        return copy(a.at[:, 0, 0:3], NXR.at[t], ns.at[t, 0], nr.at[t, 0], 0, -1)

    def rim_y(t):
        return copy(NYS.at[t], NYR.at[t], ns.at[t, 1], nr.at[t, 1], 1, -1)

    def rim_y_pack(a, t):
        for c in range(3):
            for k in range(3):
                a[c, NX, k] = NXR[t, c, k]
        for c in range(3):
            for i in range(NX + 1):
                for k in range(3):
                    NYS[t, c, i, k : k + 1, :] = a[c, i, k, 0:1, :]

    def rim_y_unpack(a, t):
        for c in range(3):
            for i in range(NX + 1):
                for k in range(3):
                    a[c, i, k, NY : NY + 1, :] = NYR[t, c, i, k : k + 1, :]

    def rim_z(t):
        return copy(NZS.at[t], NZR.at[t], ns.at[t, 2], nr.at[t, 2], 2, -1)

    def rim_z_pack(a, t):
        packed = jnp.zeros((ROWS, Z), f32)
        for c in range(3):
            for i in range(NX + 1):
                packed = jnp.where(lane == c * (NX + 1) + i, a[c, i, 0][:, 0:1], packed)
        NZS[t] = packed

    def rim_z_unpack(a, t):
        packed = NZR[t]
        for c in range(3):
            for i in range(NX + 1):
                at_ = c * (NX + 1) + i
                a[c, i, 3] = jnp.where(lane == Z - 1, packed[:, at_ : at_ + 1], pltpu.roll(a[c, i, 0], Z - 1, 1))

    def halo_copies(s, dims):
        out = []
        for d, (sb, rb) in ((0, (SX, RX)), (1, (SY, RY)), (2, (SZ, RZ))):
            if d not in dims:
                continue
            for way in range(2):
                out.append(copy(sb.at[s, way], rb.at[s, way], hs.at[s, 2 * d + way], hr.at[s, 2 * d + way], d, 1 - 2 * way))
        return out

    def send_part(s, n, d, tp, tm):
        if d == 0:
            SX[s, 0, n] = tp[(X - 1) * Y : EL]
            SX[s, 1, n] = tm[0:Y]
        else:
            for ix in range(X):
                SY[s, 0, n, ix : ix + 1] = tp[ix * Y + Y - 1 : ix * Y + Y]
                SY[s, 1, n, ix : ix + 1] = tm[ix * Y : ix * Y + 1]

    def prev_of(d, t, s, n):
        if d == 0:
            return jnp.concatenate([RX[s, 0, n], t[: ROWS - Y]], axis=0)
        if d == 1:
            parts = []
            for ix in range(X):
                parts += [RY[s, 0, n, ix : ix + 1], t[ix * Y : ix * Y + Y - 1]]
            return jnp.concatenate(parts + [t[EL:]], axis=0)
        return jnp.where(lane == 0, RZ[s, 0][:, n : n + 1], pltpu.roll(t, 1, 1))

    def next_of(d, t, s, n):
        if d == 0:
            return jnp.concatenate([t[Y:EL], RX[s, 1, n], t[EL:]], axis=0)
        if d == 1:
            parts = []
            for ix in range(X):
                parts += [t[ix * Y + 1 : ix * Y + Y], RY[s, 1, n, ix : ix + 1]]
            return jnp.concatenate(parts + [t[EL:]], axis=0)
        return jnp.where(lane == Z - 1, RZ[s, 1][:, n : n + 1], pltpu.roll(t, Z - 1, 1))

    strides = (9, 3, 1)
    others = [[m for m in range(27) if (m // strides[d]) % 3 == 0] for d in range(3)]

    def rate(src, s, first, between):
        u = [src[m] for m in range(27)]
        v = [VEL[d] for d in range(3)]
        tp, tm = [[], [], []], [[], [], []]
        for d in (2, 1, 0):
            for m in others[d]:
                even = plus_values[0] * u[m] + plus_values[2] * u[m + 2 * strides[d]]
                odd = plus_values[1] * u[m + strides[d]]
                tp[d].append(even + odd)
                tm[d].append(even - odd)
            ups = tp[d] + [v[d]]
            lows = tm[d] + [v[d]]
            if d == 2:
                up, low = jnp.zeros((ROWS, Z), f32), jnp.zeros((ROWS, Z), f32)
                for n in range(10 if first else 9):
                    up = jnp.where(lane == n, ups[n][:, Z - 1 : Z], up)
                    low = jnp.where(lane == n, lows[n][:, 0:1], low)
                SZ[s, 0] = up
                SZ[s, 1] = low
            else:
                for n in range(10):
                    send_part(s, n, d, ups[n], lows[n])
            for cp in halo_copies(s, (d,)):
                cp.start()
        acc = [None] * 27
        for d in range(3):
            st = strides[d]
            va, vb = (2.0 * g10) * v[d], (2.0 * g21) * v[d]
            for m in others[d]:
                for mm, term in ((m + st, va * u[m]), (m + 2 * st, vb * u[m + st])):
                    acc[mm] = term if acc[mm] is None else acc[mm] + term
        between()
        for d in range(3):
            for cp in halo_copies(s, (d,)):
                cp.wait()
            if first:
                high = v[d] + next_of(d, v[d], s, 9)
                lowf = prev_of(d, v[d], s, 9) + v[d]
                FS[d, 0] = jnp.maximum(high, 0.0)
                FS[d, 1] = jnp.minimum(high, 0.0)
                FS[d, 2] = jnp.maximum(lowf, 0.0)
                FS[d, 3] = jnp.minimum(lowf, 0.0)
            st = strides[d]
            hp, hm, lp, lm = [FS[d, t] for t in range(4)]
            for n, m in enumerate(others[d]):
                hi = hp * tp[d][n] + hm * next_of(d, tm[d][n], s, n)
                lo = lp * prev_of(d, tp[d][n], s, n) + lm * tm[d][n]
                diff, both = lo - hi, lo + hi
                for mm, term in (
                    (m, plus_values[0] * diff),
                    (m + st, (-plus_values[1]) * both),
                    (m + 2 * st, plus_values[2] * diff),
                ):
                    acc[mm] = term if acc[mm] is None else acc[mm] + term
        return acc

    def yz_of(src):
        def yz(i, carry):
            for c in range(3):
                yv, yd = [], []
                for k in range(4):
                    sv = sd = None
                    for j in range(NY + 1):
                        x = src[c, i, k, j : j + 1, :]
                        tv, td = tab[oTV + j] * x, tab[oTD + j] * x
                        sv = tv if sv is None else sv + tv
                        sd = td if sd is None else sd + td
                    yv.append(sv)
                    yd.append(sd)
                for r in range(4):
                    A[0, c, i, r] = sum(float(value[r, k]) * yv[k] for k in range(4))
                    A[1, c, i, r] = sum(float(value[r, k]) * yd[k] for k in range(4))
                    A[2, c, i, r] = sum(float(slope[r, k]) * yv[k] for k in range(4))
            return carry

        lax.fori_loop(0, NX + 1, yz, 0)

    def slope_at(ix, p, r, c, d):
        tb = slope if d == 0 else value
        return sum(float(tb[p, m]) * A[d, c, 3 * ix + m, r] for m in range(4))

    def jacobians(t):
        ix, r = t // 4, t % 4
        for p in range(4):
            for c in range(3):
                for d in range(3):
                    jac = slope_at(ix, p, r, c, d)
                    J[d, c, ix, p, r] = jac + 1.0 if c == d else jac

    red_start(0, 0)

    def between_0():
        red_finish(0, 0, jnp.maximum)
        red_start(0, 1)
        unweave()
        rim_x(N, 0).start()

    def between_1():
        rim_x(N, 0).wait()
        rim_y_pack(N, 0)
        rim_y(0).start()
        red_finish(0, 1, jnp.maximum)

    def between_2():
        rim_y(0).wait()
        rim_y_unpack(N, 0)
        rim_z_pack(N, 0)
        rim_z(0).start()

    def between_3():
        rim_z(0).wait()
        rim_z_unpack(N, 0)
        yz_of(N)

    def two_stages(s, first, between_a, between_b, dt_of):
        w = rate(U, s, first, between_a)
        for m in range(27):
            W[m] = w[m]
        w = rate(W, s + 1, False, between_b)
        dt = dt_of()
        half = 0.5 * dt * dt
        for m in range(27):
            U[m] = U[m] + dt * W[m] + half * w[m]

    def time_step():
        fastest = jnp.max(RED[0, 2, 0], axis=(0, 1), keepdims=True)
        DT[...] = jnp.broadcast_to(courant / jnp.maximum(fastest, 0.25), (ROWS, Z))
        return DT[...]

    two_stages(0, True, between_0, between_1, time_step)
    two_stages(2, False, between_2, between_3, lambda: DT[...])
    units = (4 * X) // (2 * SUBSTEPS - 4)

    def substep(t, carry):
        def some(s):
            def run():
                for n in range(units):
                    jacobians((s - 4) * units + n)
            return run

        two_stages(2 * t, False, some(2 * t), some(2 * t + 1), lambda: DT[...])
        return carry

    lax.fori_loop(2, SUBSTEPS, substep, 0)
    def size_of(ix, carry):
        mid = {}
        for a in range(3):
            for r in range(4):
                mid[a, r] = None
            for c in range(3):
                t = None
                for b in range(3):
                    for e in range(Y):
                        term = tab[oL + b * Y + e] * U[a * 9 + b * 3 + c, pl.ds(ix * Y + e, 1), :]
                        t = term if t is None else t + term
                for r in range(4):
                    term = float(legendre[r, c]) * t
                    mid[a, r] = term if mid[a, r] is None else mid[a, r] + term
        for p in range(4):
            for r in range(4):
                s = sum(float(legendre[p, a]) * mid[a, r] for a in range(3))
                SIZ[ix, p, r] = jnp.exp(theta_size * s)
        return carry

    lax.fori_loop(0, X, size_of, 0)

    wrow = tab[oW]
    pairs = [(d, e) for d in range(3) for e in range(d, 3)]

    def dot3(p, q, d, e):
        return p[0][d] * q[0][e] + p[1][d] * q[1][e] + p[2][d] * q[2][e]

    def gauss_weight(r):
        return jnp.where((r == 0) | (r == 3), float(weights[0]), float(weights[1]))

    def gauss(t, esum):
        ix, r = t // 4, t % 4
        for p in range(4):
            size = SIZ[ix, p, r]
            inv = 1.0 / size
            M = [[J[d, c, ix, p, r] * inv for d in range(3)] for c in range(3)]
            D = [[None] * 3 for _ in range(3)]
            metric = None
            for d, e in pairs:
                dev = dot3(M, M, d, e)
                if d == e:
                    dev = dev - 1.0
                D[d][e] = D[e][d] = dev
                sq = dev * dev if d == e else 2.0 * (dev * dev)
                metric = sq if metric is None else metric + sq
            w = wrow * (gauss_weight(r) * float(weights[p]))
            size2 = size * size
            esum = esum + w * (size2 * size) * metric
            scale = (4.0 * w) * size2
            for c in range(3):
                for d in range(3):
                    g = M[c][0] * D[0][d] + M[c][1] * D[1][d] + M[c][2] * D[2][d]
                    G[d, c, ix, p, r] = scale * g
        return esum

    zero = jnp.zeros((ROWS, Z), f32)
    esum = lax.fori_loop(0, 4 * X, gauss, zero)

    def back_c(c, carry):
        for i in range(NX + 1):
            bv = [None] * 4
            bd = [None] * 4
            for r in range(4):
                ga = []
                for d in range(3):
                    tb = slope if d == 0 else value
                    acc = None
                    for ix in range(X):
                        m = i - 3 * ix
                        if 0 <= m <= 3:
                            for p in range(4):
                                term = float(tb[p, m]) * G[d, c, ix, p, r]
                                acc = term if acc is None else acc + term
                    ga.append(acc)
                for k in range(4):
                    tv = float(value[r, k]) * ga[0] + float(slope[r, k]) * ga[2]
                    td = float(value[r, k]) * ga[1]
                    bv[k] = tv if bv[k] is None else bv[k] + tv
                    bd[k] = td if bd[k] is None else bd[k] + td
            for k in range(4):
                B[0, i, k] = bv[k]
                B[1, i, k] = bd[k]
        for i in range(NX + 1):
            for k in range(4):
                acc = None
                for s in range(ROWS):
                    term = tab[oGV + s] * B[0, i, k, s : s + 1, :] + tab[oGD + s] * B[1, i, k, s : s + 1, :]
                    acc = term if acc is None else acc + term
                GN[c, i, k] = acc
        return carry

    lax.fori_loop(0, 3, back_c, 0)

    def both_ways(src_up, src_down, axis, slot, up, down):
        copies = [
            copy(src_up, up, fs.at[slot], fr.at[slot], axis, 1),
            copy(src_down, down, fs.at[slot + 1], fr.at[slot + 1], axis, -1),
        ]
        for cp in copies:
            cp.start()
        for cp in copies:
            cp.wait()

    up, down = zero, zero
    for c in range(3):
        for i in range(NX + 1):
            here = lane == c * (NX + 1) + i
            up = jnp.where(here, GN[c, i, 3][:, Z - 1 : Z], up)
            down = jnp.where(here, GN[c, i, 0][:, 0:1], down)
    FZS[0] = up
    FZS[1] = down
    both_ways(FZS.at[0], FZS.at[1], 2, 0, FZR.at[0], FZR.at[1])
    up, down = FZR[0], FZR[1]
    for c in range(3):
        for i in range(NX + 1):
            n = c * (NX + 1) + i
            g0, g3 = GN[c, i, 0], GN[c, i, 3]
            full = g0 + jnp.where(lane == 0, up[:, n : n + 1], pltpu.roll(g3, 1, 1))
            GN[c, i, 0] = full
            GN[c, i, 3] = jnp.where(lane == Z - 1, g3 + down[:, n : n + 1], pltpu.roll(full, Z - 1, 1))
    both_ways(GN.at[:, NX], GN.at[:, 0], 0, 2, FXR.at[0], FXR.at[1])
    for c in range(3):
        for k in range(4):
            GN[c, 0, k] = GN[c, 0, k] + FXR[0, c, k]
            GN[c, NX, k] = GN[c, NX, k] + FXR[1, c, k]
    for c in range(3):
        for i in range(NX + 1):
            for k in range(4):
                FYS[0, c, i, k : k + 1, :] = GN[c, i, k, NY : NY + 1, :]
                FYS[1, c, i, k : k + 1, :] = GN[c, i, k, 0:1, :]
    both_ways(FYS.at[0], FYS.at[1], 1, 4, FYR.at[0], FYR.at[1])
    for c in range(3):
        for i in range(NX + 1):
            for k in range(4):
                GN[c, i, k, 0:1, :] = GN[c, i, k, 0:1, :] + FYR[0, c, i, k : k + 1, :]
                GN[c, i, k, NY : NY + 1, :] = GN[c, i, k, NY : NY + 1, :] + FYR[1, c, i, k : k + 1, :]
    ssum = zero
    for c in range(3):
        for i in range(NX):
            for k in range(3):
                g = GN[c, i, k]
                ssum = ssum + g * g
    ssum = jnp.where(row < NY, ssum, 0.0)
    devices = sizes[0] * sizes[1] * sizes[2]
    elements = float(EL * Z * devices)
    entries = 81.0 * elements
    mine = jnp.sum(ssum, axis=(0, 1), keepdims=True)
    bound = trial_step / jnp.sqrt(1.0 + mine / entries)
    bound = jnp.broadcast_to(bound, (ROWS, Z))
    yz_of(GN)

    def trial(t, sums):
        ix, r = t // 4, t % 4
        s1, s2, s3, s4 = sums
        for p in range(4):
            size = SIZ[ix, p, r]
            inv = 1.0 / size
            move = -(inv * bound)
            M = [[J[d, c, ix, p, r] * inv for d in range(3)] for c in range(3)]
            K = [[slope_at(ix, p, r, c, d) * move for d in range(3)] for c in range(3)]
            w = wrow * (gauss_weight(r) * float(weights[p])) * (size * size * size)
            q = [None] * 4
            for d, e in pairs:
                d0 = dot3(M, M, d, e)
                d2 = dot3(K, K, d, e)
                if d == e:
                    d0 = d0 - 1.0
                    d1 = 2.0 * dot3(M, K, d, d)
                else:
                    d1 = dot3(M, K, d, e) + dot3(K, M, d, e)
                terms = [2.0 * (d0 * d1), d1 * d1 + 2.0 * (d0 * d2), 2.0 * (d1 * d2), d2 * d2]
                for n in range(4):
                    term = terms[n] if d == e else 2.0 * terms[n]
                    q[n] = term if q[n] is None else q[n] + term
            s1, s2, s3, s4 = s1 + w * q[0], s2 + w * q[1], s3 + w * q[2], s4 + w * q[3]
        return s1, s2, s3, s4

    sums = lax.fori_loop(0, 4 * X, trial, (zero,) * 4)
    block = zero
    for n, part in enumerate((esum, ssum) + tuple(sums)):
        block = jnp.where(row == n, jnp.sum(part, axis=0, keepdims=True), block)
    column = jnp.sum(block, axis=1, keepdims=True)
    column = jnp.where(row == 6, bound, jnp.broadcast_to(column, (ROWS, Z)))
    me = (index[0] * sizes[1] + index[1]) * sizes[2] + index[2]
    groups = RED.shape[2]
    for n in range(groups):
        RED[1, 0, n] = jnp.where(lane + n * Z == me, column, 0.0)
    red_start(1, 0)
    for c in range(3):
        for k in range(3):
            slab[c * NX : (c + 1) * NX, :, k * Z : (k + 1) * Z] = GN[c, 0:NX, k]
    red_finish(1, 0, jnp.add)
    red_start(1, 1)
    woven = lax.dot_general(
        slab[...].reshape(3 * NX * ROWS, 3 * Z), perm[...], (((1,), (1,)), ((), ())),
        precision=lax.Precision.HIGHEST, preferred_element_type=f32,
    ).reshape(3, NX, ROWS, 3 * Z)
    grad[...] = woven[:, :, 0:NY, :]
    for ix in range(X):
        adv[:, ix] = U[:, ix * Y : ix * Y + Y, :]
    red_finish(1, 1, jnp.add)
    every = [RED[1, 2, n] for n in range(groups)]

    def over_all(parts):
        return sum(jnp.sum(x, axis=1, keepdims=True) for x in parts)

    etot = over_all([x[0:1] for x in every])
    stot = over_all([x[1:2] for x in every])
    step = trial_step / jnp.sqrt(1.0 + stot / entries)
    parts = []
    for n, x in enumerate(every):
        own = jnp.where(lane[0:1] + n * Z < devices, x[6:7], 1.0)
        h = step / own
        parts.append(x[0:1] + h * (x[2:3] + h * (x[3:4] + h * (x[4:5] + h * x[5:6]))))
    ttot = over_all(parts)
    l1 = lax.broadcasted_iota(jnp.int32, (1, Z), 1)
    checks[...] = jnp.where(
        l1 == 0, etot / elements, jnp.where(l1 == 1, stot / entries, ttot / elements)
    )


def solution(mesh):
    sizes = tuple(mesh.shape[a] for a in AXES)

    def on_device(displacement, size_field_modes, velocity):
        modes, X, Y, Z = size_field_modes.shape
        assert Y == 2 and displacement.shape == (3, 3 * X, 3 * Y, 3 * Z)
        R, NX, NY = 4 * Y, 3 * X, 3 * Y
        tab = jnp.asarray(row_tables(Y, Z))
        peers = sizes[0] - 1 + sizes[1] * sizes[2] - 1
        groups = -(-sizes[0] * sizes[1] * sizes[2] // Z)
        S = 2 * SUBSTEPS
        vm = lambda *shape: pltpu.VMEM(shape, jnp.float32)
        dma = lambda *shape: pltpu.SemaphoreType.DMA(shape)
        spec = pl.BlockSpec(memory_space=pltpu.VMEM)
        adv, grad, checks = pl.pallas_call(
            functools.partial(kernel, sizes, X, Y, Z),
            out_shape=(
                jax.ShapeDtypeStruct(size_field_modes.shape, jnp.float32),
                jax.ShapeDtypeStruct(displacement.shape, jnp.float32),
                jax.ShapeDtypeStruct((1, Z), jnp.float32),
            ),
            in_specs=[spec] * 4,
            out_specs=(spec,) * 3,
            scratch_shapes=[
                vm(3 * Z, 3 * Z), vm(3 * NX, R, 3 * Z), vm(27, R, Z), vm(27, R, Z), vm(3, R, Z), vm(3, 4, R, Z),
                vm(S, 2, 10, Y, Z), vm(S, 2, 10, Y, Z), vm(S, 2, 10, X, Z), vm(S, 2, 10, X, Z),
                vm(S, 2, R, Z), vm(S, 2, R, Z),
                vm(2, 3, groups, R, Z), vm(2, peers, groups, R, Z),
                vm(3, NX + 1, 4, R, Z), vm(3, NX + 1, 4, R, Z),
                vm(3, 3, NX + 1, 4, R, Z), vm(3, 3, X, 4, 4, R, Z), vm(3, 3, X, 4, 4, R, Z), vm(2, NX + 1, 4, R, Z), vm(X, 4, 4, R, Z), vm(R, Z),
                vm(1, 3, 3, R, Z), vm(1, 3, NX + 1, 3, Z), vm(1, 3, NX + 1, 3, Z), vm(1, R, Z), vm(1, R, Z),
                vm(2, 3, 4, R, Z), vm(2, 3, NX + 1, 4, Z), vm(2, 3, NX + 1, 4, Z), vm(2, R, Z), vm(2, R, Z),
                dma(S, 6), dma(S, 6), dma(2, peers), dma(2, peers), dma(1, 3), dma(1, 3), dma(6), dma(6),
            ],
            compiler_params=pltpu.CompilerParams(collective_id=0, has_side_effects=True),
        )(displacement, size_field_modes, velocity, tab)
        return adv, grad, checks[0, 0:3]

    return jax.shard_map(
        on_device,
        mesh=mesh,
        in_specs=(P(None, "gx", "gy", "gz"),) * 3,
        out_specs=(P(None, "gx", "gy", "gz"), P(None, "gx", "gy", "gz"), P()),
        check_vma=False,
    )
```

```python
import functools

import jax
import jax.numpy as jnp
import numpy as np
from jax import lax
from jax.experimental import pallas as pl
from jax.experimental.pallas import tpu as pltpu
from jax.sharding import PartitionSpec as P

SUBSTEPS = 4
MESH = pl.DeviceIdType.MESH
AXES = ("gx", "gy", "gz")

plus_values = (0.7071067811865476, 1.224744871391589, 1.5811388300841898)
g10 = 1.7320508075688772
g21 = 3.872983346207417
courant = 0.1
theta_size = 0.3
trial_step = 0.05


def tables_1d():
    points = np.array(
        [-0.8611363115940526, -0.3399810435848563, 0.3399810435848563, 0.8611363115940526]
    )
    weights = np.array(
        [0.3478548451374538, 0.6521451548625461, 0.6521451548625461, 0.3478548451374538]
    )
    points = 0.5 * (points + 1.0)
    weights = 0.5 * weights
    nodes = np.array([0.0, 1.0 / 3.0, 2.0 / 3.0, 1.0])
    value = np.zeros((4, 4))
    slope = np.zeros((4, 4))
    for m in range(4):
        others = [nodes[o] for o in range(4) if o != m]
        den = np.prod([nodes[m] - o for o in others])
        for q in range(4):
            g = points[q]
            value[q, m] = np.prod([g - o for o in others]) / den
            slope[q, m] = (
                sum(np.prod([g - others[t] for t in range(3) if t != s]) for s in range(3)) / den
            )
    c = 2.0 * points - 1.0
    legendre = np.stack(
        [
            np.full(4, plus_values[0]),
            plus_values[1] * c,
            plus_values[2] * 0.5 * (3.0 * c**2 - 1.0),
        ],
        axis=1,
    )
    return value, slope, legendre, weights


def row_tables(Y, Z):
    value, slope, legendre, weights = tables_1d()
    rows, nodes = 4 * Y, 3 * Y + 1
    tv = np.zeros((rows, rows))
    td = np.zeros((rows, rows))
    for e in range(Y):
        tv[4 * e : 4 * e + 4, 3 * e : 3 * e + 4] = value
        td[4 * e : 4 * e + 4, 3 * e : 3 * e + 4] = slope
    blocks = [tv[:, j] for j in range(nodes)] + [td[:, j] for j in range(nodes)]
    blocks += [tv[s, :] for s in range(rows)] + [td[s, :] for s in range(rows)]
    for b in range(3):
        for e in range(Y):
            col = np.zeros(rows)
            col[4 * e : 4 * e + 4] = legendre[:, b]
            blocks.append(col)
    blocks.append(np.tile(weights, Y))
    stacked = np.stack(blocks).astype(np.float32)
    return np.ascontiguousarray(np.broadcast_to(stacked[:, :, None], stacked.shape + (Z,)))


def kernel(sizes, X, Y, Z, disp, modes, vel, tab, adv, grad, checks,
           perm, slab, U, W, VEL, FS, SX, RX, SY, RY, SZ, RZ,
           RED, REDR, N, GN, A, G, J, B, SIZ, DT,
           NXR, NYS, NYR, NZS, NZR, FXR, FYS, FYR, FZS, FZR,
           hs, hr, rs, rr, ns, nr, fs, fr):
    value, slope, legendre, weights = tables_1d()
    NX, NY = 3 * X, 3 * Y
    ROWS = 4 * Y
    EL = X * Y
    f32 = jnp.float32
    index = [lax.axis_index(a) for a in AXES]
    lane = lax.broadcasted_iota(jnp.int32, (ROWS, Z), 1)
    row = lax.broadcasted_iota(jnp.int32, (ROWS, Z), 0)
    oTV, oTD, oGV, oGD, oL, oW = 0, NY + 1, 2 * NY + 2, 2 * NY + 2 + ROWS, 2 * NY + 2 + 2 * ROWS, 2 * NY + 2 + 2 * ROWS + 3 * Y

    def at(axis, by):
        n = sizes[axis]
        return {AXES[axis]: lax.rem(index[axis] + (by + n), n)}

    barrier = pltpu.get_barrier_semaphore()
    total = 0
    moves = [(by, 0, 0) for by in range(1, sizes[0])]
    moves += [(0, b, c) for b in range(sizes[1]) for c in range(sizes[2]) if b or c]
    for move in moves:
        target = {}
        for axis in range(3):
            if move[axis]:
                target.update(at(axis, move[axis]))
        pl.semaphore_signal(barrier, inc=1, device_id=target, device_id_type=MESH)
        total += 1

    def copy(src, dst, ss, sr, axis, by):
        return pltpu.make_async_remote_copy(
            src_ref=src, dst_ref=dst, send_sem=ss, recv_sem=sr,
            device_id=at(axis, by), device_id_type=MESH,
        )

    U[...] = jnp.zeros_like(U)
    VEL[...] = jnp.zeros_like(VEL)
    for ix in range(X):
        U[:, ix * Y : ix * Y + Y, :] = modes[:, ix]
        VEL[:, ix * Y : ix * Y + Y, :] = vel[:, ix]
    RED[0, 0] = jnp.zeros_like(RED[0, 0])
    RED[0, 0, 0] = jnp.abs(VEL[0]) + jnp.abs(VEL[1]) + jnp.abs(VEL[2])
    def unweave():
        a_i = lax.broadcasted_iota(jnp.int32, (3 * Z, 3 * Z), 0)
        b_i = lax.broadcasted_iota(jnp.int32, (3 * Z, 3 * Z), 1)
        b_k = (b_i >= Z).astype(jnp.int32) + (b_i >= 2 * Z).astype(jnp.int32)
        perm[...] = (a_i == 3 * (b_i - b_k * Z) + b_k).astype(f32)
        slab[...] = jnp.zeros_like(slab)
        for c in range(3):
            for i in range(NX):
                slab[c * NX + i, 0:NY, :] = disp[c, i]
        spread = jnp.dot(
            slab[...].reshape(3 * NX * ROWS, 3 * Z), perm[...],
            precision=lax.Precision.HIGHEST, preferred_element_type=f32,
        ).reshape(3, NX, ROWS, 3 * Z)
        for c in range(3):
            for k in range(3):
                N[c, 0:NX, k] = spread[c, :, :, k * Z : (k + 1) * Z]

    pl.semaphore_wait(barrier, total)

    def peers_of(phase):
        if phase == 0:
            return [(by, 0, 0) for by in range(1, sizes[0])]
        return [(0, b, c) for b in range(sizes[1]) for c in range(sizes[2]) if b or c]

    def red_copies(r, phase):
        off = 0 if phase == 0 else sizes[0] - 1
        out = []
        for n, move in enumerate(peers_of(phase)):
            target = {}
            for axis in range(3):
                if move[axis]:
                    target.update(at(axis, move[axis]))
            out.append(pltpu.make_async_remote_copy(
                src_ref=RED.at[r, phase], dst_ref=REDR.at[r, off + n],
                send_sem=rs.at[r, off + n], recv_sem=rr.at[r, off + n],
                device_id=target, device_id_type=MESH,
            ))
        return out

    def red_start(r, phase):
        for cp in red_copies(r, phase):
            cp.start()

    def red_finish(r, phase, op):
        off = 0 if phase == 0 else sizes[0] - 1
        copies = red_copies(r, phase)
        for cp in copies:
            cp.wait_recv()
        total = RED[r, phase]
        for n in range(len(copies)):
            total = op(total, REDR[r, off + n])
        RED[r, phase + 1] = total

    def rim_x(a, t):
        return copy(a.at[:, 0, 0:3], NXR.at[t], ns.at[t, 0], nr.at[t, 0], 0, -1)

    def rim_y(t):
        return copy(NYS.at[t], NYR.at[t], ns.at[t, 1], nr.at[t, 1], 1, -1)

    def rim_y_pack(a, t):
        for c in range(3):
            for k in range(3):
                a[c, NX, k] = NXR[t, c, k]
        for c in range(3):
            for i in range(NX + 1):
                for k in range(3):
                    NYS[t, c, i, k : k + 1, :] = a[c, i, k, 0:1, :]

    def rim_y_unpack(a, t):
        for c in range(3):
            for i in range(NX + 1):
                for k in range(3):
                    a[c, i, k, NY : NY + 1, :] = NYR[t, c, i, k : k + 1, :]

    def rim_z(t):
        return copy(NZS.at[t], NZR.at[t], ns.at[t, 2], nr.at[t, 2], 2, -1)

    def rim_z_pack(a, t):
        packed = jnp.zeros((ROWS, Z), f32)
        for c in range(3):
            for i in range(NX + 1):
                packed = jnp.where(lane == c * (NX + 1) + i, a[c, i, 0][:, 0:1], packed)
        NZS[t] = packed

    def rim_z_unpack(a, t):
        packed = NZR[t]
        for c in range(3):
            for i in range(NX + 1):
                at_ = c * (NX + 1) + i
                a[c, i, 3] = jnp.where(lane == Z - 1, packed[:, at_ : at_ + 1], pltpu.roll(a[c, i, 0], Z - 1, 1))

    def halo_copies(s, dims):
        out = []
        for d, (sb, rb) in ((0, (SX, RX)), (1, (SY, RY)), (2, (SZ, RZ))):
            if d not in dims:
                continue
            for way in range(2):
                out.append(copy(sb.at[s, way], rb.at[s, way], hs.at[s, 2 * d + way], hr.at[s, 2 * d + way], d, 1 - 2 * way))
        return out

    def send_part(s, n, d, tp, tm):
        if d == 0:
            SX[s, 0, n] = tp[(X - 1) * Y : EL]
            SX[s, 1, n] = tm[0:Y]
        else:
            for ix in range(X):
                SY[s, 0, n, ix : ix + 1] = tp[ix * Y + Y - 1 : ix * Y + Y]
                SY[s, 1, n, ix : ix + 1] = tm[ix * Y : ix * Y + 1]

    def prev_of(d, t, s, n):
        if d == 0:
            return jnp.concatenate([RX[s, 0, n], t[: ROWS - Y]], axis=0)
        if d == 1:
            parts = []
            for ix in range(X):
                parts += [RY[s, 0, n, ix : ix + 1], t[ix * Y : ix * Y + Y - 1]]
            return jnp.concatenate(parts + [t[EL:]], axis=0)
        return jnp.where(lane == 0, RZ[s, 0][:, n : n + 1], pltpu.roll(t, 1, 1))

    def next_of(d, t, s, n):
        if d == 0:
            return jnp.concatenate([t[Y:EL], RX[s, 1, n], t[EL:]], axis=0)
        if d == 1:
            parts = []
            for ix in range(X):
                parts += [t[ix * Y + 1 : ix * Y + Y], RY[s, 1, n, ix : ix + 1]]
            return jnp.concatenate(parts + [t[EL:]], axis=0)
        return jnp.where(lane == Z - 1, RZ[s, 1][:, n : n + 1], pltpu.roll(t, Z - 1, 1))

    strides = (9, 3, 1)
    others = [[m for m in range(27) if (m // strides[d]) % 3 == 0] for d in range(3)]

    def rate(src, s, first, between):
        u = [src[m] for m in range(27)]
        v = [VEL[d] for d in range(3)]
        tp, tm = [[], [], []], [[], [], []]
        for d in (2, 1, 0):
            for m in others[d]:
                even = plus_values[0] * u[m] + plus_values[2] * u[m + 2 * strides[d]]
                odd = plus_values[1] * u[m + strides[d]]
                tp[d].append(even + odd)
                tm[d].append(even - odd)
            ups = tp[d] + [v[d]]
            lows = tm[d] + [v[d]]
            if d == 2:
                up, low = jnp.zeros((ROWS, Z), f32), jnp.zeros((ROWS, Z), f32)
                for n in range(10 if first else 9):
                    up = jnp.where(lane == n, ups[n][:, Z - 1 : Z], up)
                    low = jnp.where(lane == n, lows[n][:, 0:1], low)
                SZ[s, 0] = up
                SZ[s, 1] = low
            else:
                for n in range(10):
                    send_part(s, n, d, ups[n], lows[n])
            for cp in halo_copies(s, (d,)):
                cp.start()
        acc = [None] * 27
        for d in range(3):
            st = strides[d]
            va, vb = (2.0 * g10) * v[d], (2.0 * g21) * v[d]
            for m in others[d]:
                for mm, term in ((m + st, va * u[m]), (m + 2 * st, vb * u[m + st])):
                    acc[mm] = term if acc[mm] is None else acc[mm] + term
        between()
        for d in range(3):
            for cp in halo_copies(s, (d,)):
                cp.wait_recv()
            if first:
                high = v[d] + next_of(d, v[d], s, 9)
                lowf = prev_of(d, v[d], s, 9) + v[d]
                FS[d, 0] = jnp.maximum(high, 0.0)
                FS[d, 1] = jnp.minimum(high, 0.0)
                FS[d, 2] = jnp.maximum(lowf, 0.0)
                FS[d, 3] = jnp.minimum(lowf, 0.0)
            st = strides[d]
            hp, hm, lp, lm = [FS[d, t] for t in range(4)]
            for n, m in enumerate(others[d]):
                hi = hp * tp[d][n] + hm * next_of(d, tm[d][n], s, n)
                lo = lp * prev_of(d, tp[d][n], s, n) + lm * tm[d][n]
                diff, both = lo - hi, lo + hi
                for mm, term in (
                    (m, plus_values[0] * diff),
                    (m + st, (-plus_values[1]) * both),
                    (m + 2 * st, plus_values[2] * diff),
                ):
                    acc[mm] = term if acc[mm] is None else acc[mm] + term
        return acc

    def yz_of(src):
        def yz(i, carry):
            for c in range(3):
                yv, yd = [], []
                for k in range(4):
                    sv = sd = None
                    for j in range(NY + 1):
                        x = src[c, i, k, j : j + 1, :]
                        tv, td = tab[oTV + j] * x, tab[oTD + j] * x
                        sv = tv if sv is None else sv + tv
                        sd = td if sd is None else sd + td
                    yv.append(sv)
                    yd.append(sd)
                for r in range(4):
                    A[0, c, i, r] = sum(float(value[r, k]) * yv[k] for k in range(4))
                    A[1, c, i, r] = sum(float(value[r, k]) * yd[k] for k in range(4))
                    A[2, c, i, r] = sum(float(slope[r, k]) * yv[k] for k in range(4))
            return carry

        lax.fori_loop(0, NX + 1, yz, 0)

    def slope_at(ix, p, r, c, d):
        tb = slope if d == 0 else value
        return sum(float(tb[p, m]) * A[d, c, 3 * ix + m, r] for m in range(4))

    def jacobians(t):
        ix, r = t // 4, t % 4
        for p in range(4):
            for c in range(3):
                for d in range(3):
                    jac = slope_at(ix, p, r, c, d)
                    J[d, c, ix, p, r] = jac + 1.0 if c == d else jac

    red_start(0, 0)

    def between_0():
        red_finish(0, 0, jnp.maximum)
        red_start(0, 1)
        unweave()
        rim_x(N, 0).start()

    def between_1():
        rim_x(N, 0).wait()
        rim_y_pack(N, 0)
        rim_y(0).start()
        red_finish(0, 1, jnp.maximum)

    def between_2():
        rim_y(0).wait()
        rim_y_unpack(N, 0)
        rim_z_pack(N, 0)
        rim_z(0).start()

    def between_3():
        rim_z(0).wait()
        rim_z_unpack(N, 0)
        yz_of(N)

    def two_stages(s, first, between_a, between_b, dt_of):
        w = rate(U, s, first, between_a)
        for m in range(27):
            W[m] = w[m]
        w = rate(W, s + 1, False, between_b)
        dt = dt_of()
        half = 0.5 * dt * dt
        for m in range(27):
            U[m] = U[m] + dt * W[m] + half * w[m]

    def time_step():
        fastest = jnp.max(RED[0, 2, 0], axis=(0, 1), keepdims=True)
        DT[...] = jnp.broadcast_to(courant / jnp.maximum(fastest, 0.25), (ROWS, Z))
        return DT[...]

    two_stages(0, True, between_0, between_1, time_step)
    two_stages(2, False, between_2, between_3, lambda: DT[...])
    units = (4 * X) // (2 * SUBSTEPS - 4)

    def substep(t, carry):
        def some(s):
            def run():
                for n in range(units):
                    jacobians((s - 4) * units + n)
            return run

        two_stages(2 * t, False, some(2 * t), some(2 * t + 1), lambda: DT[...])
        return carry

    lax.fori_loop(2, SUBSTEPS, substep, 0)
    def size_of(ix, carry):
        mid = {}
        for a in range(3):
            for r in range(4):
                mid[a, r] = None
            for c in range(3):
                t = None
                for b in range(3):
                    for e in range(Y):
                        term = tab[oL + b * Y + e] * U[a * 9 + b * 3 + c, pl.ds(ix * Y + e, 1), :]
                        t = term if t is None else t + term
                for r in range(4):
                    term = float(legendre[r, c]) * t
                    mid[a, r] = term if mid[a, r] is None else mid[a, r] + term
        for p in range(4):
            for r in range(4):
                s = sum(float(legendre[p, a]) * mid[a, r] for a in range(3))
                SIZ[ix, p, r] = jnp.exp(theta_size * s)
        return carry

    lax.fori_loop(0, X, size_of, 0)

    wrow = tab[oW]
    pairs = [(d, e) for d in range(3) for e in range(d, 3)]

    def dot3(p, q, d, e):
        return p[0][d] * q[0][e] + p[1][d] * q[1][e] + p[2][d] * q[2][e]

    def gauss_weight(r):
        return jnp.where((r == 0) | (r == 3), float(weights[0]), float(weights[1]))

    def gauss(t, esum):
        ix, r = t // 4, t % 4
        for p in range(4):
            size = SIZ[ix, p, r]
            inv = 1.0 / size
            M = [[J[d, c, ix, p, r] * inv for d in range(3)] for c in range(3)]
            D = [[None] * 3 for _ in range(3)]
            metric = None
            for d, e in pairs:
                dev = dot3(M, M, d, e)
                if d == e:
                    dev = dev - 1.0
                D[d][e] = D[e][d] = dev
                sq = dev * dev if d == e else 2.0 * (dev * dev)
                metric = sq if metric is None else metric + sq
            w = wrow * (gauss_weight(r) * float(weights[p]))
            size2 = size * size
            esum = esum + w * (size2 * size) * metric
            scale = (4.0 * w) * size2
            for c in range(3):
                for d in range(3):
                    g = M[c][0] * D[0][d] + M[c][1] * D[1][d] + M[c][2] * D[2][d]
                    G[d, c, ix, p, r] = scale * g
        return esum

    zero = jnp.zeros((ROWS, Z), f32)
    esum = lax.fori_loop(0, 4 * X, gauss, zero)

    def back_c(c, carry):
        for i in range(NX + 1):
            bv = [None] * 4
            bd = [None] * 4
            for r in range(4):
                ga = []
                for d in range(3):
                    tb = slope if d == 0 else value
                    acc = None
                    for ix in range(X):
                        m = i - 3 * ix
                        if 0 <= m <= 3:
                            for p in range(4):
                                term = float(tb[p, m]) * G[d, c, ix, p, r]
                                acc = term if acc is None else acc + term
                    ga.append(acc)
                for k in range(4):
                    tv = float(value[r, k]) * ga[0] + float(slope[r, k]) * ga[2]
                    td = float(value[r, k]) * ga[1]
                    bv[k] = tv if bv[k] is None else bv[k] + tv
                    bd[k] = td if bd[k] is None else bd[k] + td
            for k in range(4):
                B[0, i, k] = bv[k]
                B[1, i, k] = bd[k]
        for i in range(NX + 1):
            for k in range(4):
                acc = None
                for s in range(ROWS):
                    term = tab[oGV + s] * B[0, i, k, s : s + 1, :] + tab[oGD + s] * B[1, i, k, s : s + 1, :]
                    acc = term if acc is None else acc + term
                GN[c, i, k] = acc
        return carry

    lax.fori_loop(0, 3, back_c, 0)

    def both_ways(src_up, src_down, axis, slot, up, down):
        copies = [
            copy(src_up, up, fs.at[slot], fr.at[slot], axis, 1),
            copy(src_down, down, fs.at[slot + 1], fr.at[slot + 1], axis, -1),
        ]
        for cp in copies:
            cp.start()
        for cp in copies:
            cp.wait()

    up, down = zero, zero
    for c in range(3):
        for i in range(NX + 1):
            here = lane == c * (NX + 1) + i
            up = jnp.where(here, GN[c, i, 3][:, Z - 1 : Z], up)
            down = jnp.where(here, GN[c, i, 0][:, 0:1], down)
    FZS[0] = up
    FZS[1] = down
    both_ways(FZS.at[0], FZS.at[1], 2, 0, FZR.at[0], FZR.at[1])
    up, down = FZR[0], FZR[1]
    for c in range(3):
        for i in range(NX + 1):
            n = c * (NX + 1) + i
            g0, g3 = GN[c, i, 0], GN[c, i, 3]
            full = g0 + jnp.where(lane == 0, up[:, n : n + 1], pltpu.roll(g3, 1, 1))
            GN[c, i, 0] = full
            GN[c, i, 3] = jnp.where(lane == Z - 1, g3 + down[:, n : n + 1], pltpu.roll(full, Z - 1, 1))
    both_ways(GN.at[:, NX], GN.at[:, 0], 0, 2, FXR.at[0], FXR.at[1])
    for c in range(3):
        for k in range(4):
            GN[c, 0, k] = GN[c, 0, k] + FXR[0, c, k]
            GN[c, NX, k] = GN[c, NX, k] + FXR[1, c, k]
    for c in range(3):
        for i in range(NX + 1):
            for k in range(4):
                FYS[0, c, i, k : k + 1, :] = GN[c, i, k, NY : NY + 1, :]
                FYS[1, c, i, k : k + 1, :] = GN[c, i, k, 0:1, :]
    both_ways(FYS.at[0], FYS.at[1], 1, 4, FYR.at[0], FYR.at[1])
    for c in range(3):
        for i in range(NX + 1):
            for k in range(4):
                GN[c, i, k, 0:1, :] = GN[c, i, k, 0:1, :] + FYR[0, c, i, k : k + 1, :]
                GN[c, i, k, NY : NY + 1, :] = GN[c, i, k, NY : NY + 1, :] + FYR[1, c, i, k : k + 1, :]
    ssum = zero
    for c in range(3):
        for i in range(NX):
            for k in range(3):
                g = GN[c, i, k]
                ssum = ssum + g * g
    ssum = jnp.where(row < NY, ssum, 0.0)
    devices = sizes[0] * sizes[1] * sizes[2]
    elements = float(EL * Z * devices)
    entries = 81.0 * elements
    mine = jnp.sum(ssum, axis=(0, 1), keepdims=True)
    bound = trial_step / jnp.sqrt(1.0 + mine / entries)
    bound = jnp.broadcast_to(bound, (ROWS, Z))
    yz_of(GN)

    def trial(t, sums):
        ix, r = t // 4, t % 4
        s1, s2, s3, s4 = sums
        for p in range(4):
            size = SIZ[ix, p, r]
            inv = 1.0 / size
            move = -(inv * bound)
            M = [[J[d, c, ix, p, r] * inv for d in range(3)] for c in range(3)]
            K = [[slope_at(ix, p, r, c, d) * move for d in range(3)] for c in range(3)]
            w = wrow * (gauss_weight(r) * float(weights[p])) * (size * size * size)
            q = [None] * 4
            for d, e in pairs:
                d0 = dot3(M, M, d, e)
                d2 = dot3(K, K, d, e)
                if d == e:
                    d0 = d0 - 1.0
                    d1 = 2.0 * dot3(M, K, d, d)
                else:
                    d1 = dot3(M, K, d, e) + dot3(K, M, d, e)
                terms = [2.0 * (d0 * d1), d1 * d1 + 2.0 * (d0 * d2), 2.0 * (d1 * d2), d2 * d2]
                for n in range(4):
                    term = terms[n] if d == e else 2.0 * terms[n]
                    q[n] = term if q[n] is None else q[n] + term
            s1, s2, s3, s4 = s1 + w * q[0], s2 + w * q[1], s3 + w * q[2], s4 + w * q[3]
        return s1, s2, s3, s4

    sums = lax.fori_loop(0, 4 * X, trial, (zero,) * 4)
    block = zero
    for n, part in enumerate((esum, ssum) + tuple(sums)):
        block = jnp.where(row == n, jnp.sum(part, axis=0, keepdims=True), block)
    column = jnp.sum(block, axis=1, keepdims=True)
    column = jnp.where(row == 6, bound, jnp.broadcast_to(column, (ROWS, Z)))
    me = (index[0] * sizes[1] + index[1]) * sizes[2] + index[2]
    groups = RED.shape[2]
    for n in range(groups):
        RED[1, 0, n] = jnp.where(lane + n * Z == me, column, 0.0)
    red_start(1, 0)
    for c in range(3):
        for k in range(3):
            slab[c * NX : (c + 1) * NX, :, k * Z : (k + 1) * Z] = GN[c, 0:NX, k]
    red_finish(1, 0, jnp.add)
    red_start(1, 1)
    woven = lax.dot_general(
        slab[...].reshape(3 * NX * ROWS, 3 * Z), perm[...], (((1,), (1,)), ((), ())),
        precision=lax.Precision.HIGHEST, preferred_element_type=f32,
    ).reshape(3, NX, ROWS, 3 * Z)
    grad[...] = woven[:, :, 0:NY, :]
    for ix in range(X):
        adv[:, ix] = U[:, ix * Y : ix * Y + Y, :]
    red_finish(1, 1, jnp.add)
    every = [RED[1, 2, n] for n in range(groups)]

    def over_all(parts):
        return sum(jnp.sum(x, axis=1, keepdims=True) for x in parts)

    etot = over_all([x[0:1] for x in every])
    stot = over_all([x[1:2] for x in every])
    step = trial_step / jnp.sqrt(1.0 + stot / entries)
    parts = []
    for n, x in enumerate(every):
        own = jnp.where(lane[0:1] + n * Z < devices, x[6:7], 1.0)
        h = step / own
        parts.append(x[0:1] + h * (x[2:3] + h * (x[3:4] + h * (x[4:5] + h * x[5:6]))))
    ttot = over_all(parts)
    for t in range(2 * SUBSTEPS):
        for cp in halo_copies(t, (0, 1, 2)):
            cp.wait_send()
    for r in range(2):
        for phase in range(2):
            for cp in red_copies(r, phase):
                cp.wait_send()
    l1 = lax.broadcasted_iota(jnp.int32, (1, Z), 1)
    checks[...] = jnp.where(
        l1 == 0, etot / elements, jnp.where(l1 == 1, stot / entries, ttot / elements)
    )


def solution(mesh):
    sizes = tuple(mesh.shape[a] for a in AXES)

    def on_device(displacement, size_field_modes, velocity):
        modes, X, Y, Z = size_field_modes.shape
        assert Y == 2 and displacement.shape == (3, 3 * X, 3 * Y, 3 * Z)
        R, NX, NY = 4 * Y, 3 * X, 3 * Y
        tab = jnp.asarray(row_tables(Y, Z))
        peers = sizes[0] - 1 + sizes[1] * sizes[2] - 1
        groups = -(-sizes[0] * sizes[1] * sizes[2] // Z)
        S = 2 * SUBSTEPS
        vm = lambda *shape: pltpu.VMEM(shape, jnp.float32)
        dma = lambda *shape: pltpu.SemaphoreType.DMA(shape)
        spec = pl.BlockSpec(memory_space=pltpu.VMEM)
        adv, grad, checks = pl.pallas_call(
            functools.partial(kernel, sizes, X, Y, Z),
            out_shape=(
                jax.ShapeDtypeStruct(size_field_modes.shape, jnp.float32),
                jax.ShapeDtypeStruct(displacement.shape, jnp.float32),
                jax.ShapeDtypeStruct((1, Z), jnp.float32),
            ),
            in_specs=[spec] * 4,
            out_specs=(spec,) * 3,
            scratch_shapes=[
                vm(3 * Z, 3 * Z), vm(3 * NX, R, 3 * Z), vm(27, R, Z), vm(27, R, Z), vm(3, R, Z), vm(3, 4, R, Z),
                vm(S, 2, 10, Y, Z), vm(S, 2, 10, Y, Z), vm(S, 2, 10, X, Z), vm(S, 2, 10, X, Z),
                vm(S, 2, R, Z), vm(S, 2, R, Z),
                vm(2, 3, groups, R, Z), vm(2, peers, groups, R, Z),
                vm(3, NX + 1, 4, R, Z), vm(3, NX + 1, 4, R, Z),
                vm(3, 3, NX + 1, 4, R, Z), vm(3, 3, X, 4, 4, R, Z), vm(3, 3, X, 4, 4, R, Z), vm(2, NX + 1, 4, R, Z), vm(X, 4, 4, R, Z), vm(R, Z),
                vm(1, 3, 3, R, Z), vm(1, 3, NX + 1, 3, Z), vm(1, 3, NX + 1, 3, Z), vm(1, R, Z), vm(1, R, Z),
                vm(2, 3, 4, R, Z), vm(2, 3, NX + 1, 4, Z), vm(2, 3, NX + 1, 4, Z), vm(2, R, Z), vm(2, R, Z),
                dma(S, 6), dma(S, 6), dma(2, peers), dma(2, peers), dma(1, 3), dma(1, 3), dma(6), dma(6),
            ],
            compiler_params=pltpu.CompilerParams(collective_id=0, has_side_effects=True),
        )(displacement, size_field_modes, velocity, tab)
        return adv, grad, checks[0, 0:3]

    return jax.shard_map(
        on_device,
        mesh=mesh,
        in_specs=(P(None, "gx", "gy", "gz"),) * 3,
        out_specs=(P(None, "gx", "gy", "gz"), P(None, "gx", "gy", "gz"), P()),
        check_vma=False,
    )
```
